32 devices in a mesh: row: 16 (over z, x, core), col: 2 (over y).
Axes of the slice: x: 2, y: 2, z: 4, core: 2. Of those that a mesh axis runs over, the one named last changes fastest.
Arguments:
- joined: bfloat16 [2, 64, 16, 28, 4096], P(None, None, 'row', None, 'col'), may hold values from -0.09375 to 0.09375
- probes: bfloat16 [2, 128, 4096], P(None, None, 'col'), may hold values from -6 to 6
Outputs:
- gate_rows: bfloat16 [2, 14336, 4096], P(None, 'row', 'col')
- up_rows: bfloat16 [2, 14336, 4096], P(None, 'row', 'col')
- hidden: bfloat16 [2, 128, 14336], P(None, 'col', 'row')
The draws below stay inside these ranges and needn't reach their ends.
All inputs are finite; a program needn't handle non-finite values.
Results may differ from the reference program's by a relative error of at most 0.002.
Values may be sent and summed in bfloat16 or wider, within the bound.
A program may use at most 128 MiB of HBM per device.

```python
import jax
import jax.numpy as jnp

D = 4096
FF = 14336
HALF = 14
LAYERS = 2
TOKENS = 128
CYCLES = 64
N_ROW = 16


def block_levels(rng, dims, split, least, largest):
    factor_of = 1.0
    for dim, blocks in split:
        heights = jax.random.uniform(jax.random.fold_in(jax.random.fold_in(rng, 6), dim), (blocks,), jnp.float32, least / len(split), largest / len(split))
        factor_of = factor_of * jnp.repeat(jnp.exp(heights), dims[dim] // blocks).reshape((-1,) + (1,) * (len(dims) - 1 - dim))
    return factor_of


def gaussian(rng, extent, deviation, reach, split=(), held_as=jnp.bfloat16):
    values = deviation * jax.random.normal(rng, extent, jnp.float32)
    if split:
        values = values * block_levels(rng, extent, split, -0.22, 0.18)
    return jnp.clip(values, -reach, reach).astype(held_as)


def setup_inputs(seed: int = 0) -> dict:
    splits = jax.random.split(jax.random.key(seed), 3)
    return {
        "joined": gaussian(splits[0], (LAYERS, CYCLES, N_ROW, 2 * HALF, D), D ** -0.5, 0.09375, ((2, 16), (4, 2))),
        "probes": gaussian(splits[1], (LAYERS, TOKENS, D), 1.0, 6.0, ((2, 2),)),
    }


def reference(joined, probes):
    blocks = joined.reshape(LAYERS, CYCLES * N_ROW, HALF, 2, D)
    gate_rows = blocks[:, :, :, 0, :].reshape(LAYERS, FF, D)
    up_rows = blocks[:, :, :, 1, :].reshape(LAYERS, FF, D)
    results = []
    for layer_index in range(LAYERS):
        gate_proj = jnp.dot(probes[layer_index], gate_rows[layer_index].T, preferred_element_type=jnp.float32)
        up_proj = jnp.dot(probes[layer_index], up_rows[layer_index].T, preferred_element_type=jnp.float32)
        results.append((jax.nn.silu(gate_proj) * up_proj).astype(jnp.bfloat16))
    hidden = jnp.stack(results, axis=0)
    return gate_rows, up_rows, hidden
```

```python
import functools

import jax
import jax.numpy as jnp
import numpy as np
from jax import lax
from jax.experimental import pallas as pl
from jax.experimental.pallas import tpu as pltpu
from jax.sharding import PartitionSpec as P

MESH = pl.DeviceIdType.MESH
BAND = 16
PEERS = 8


def pack_matrix(groups, block_rows, slot):
    half = block_rows // 2
    dests = BAND // groups
    out = np.zeros((dests * slot, block_rows * BAND), np.float32)
    for q in range(dests):
        for h in range(2):
            for g in range(groups):
                for r in range(half):
                    out[q * slot + (h * groups + g) * half + r, (2 * r + h) * BAND + q * groups + g] = 1
    return out


def unpack_matrix(groups, block_rows, slot):
    half = block_rows // 2
    out = np.zeros((2 * groups * PEERS * half, PEERS * slot), np.float32)
    for h in range(2):
        for g in range(groups):
            for p in range(PEERS):
                for r in range(half):
                    out[((h * groups + g) * PEERS + p) * half + r, p * slot + (h * groups + g) * half + r] = 1
    return out


def kernel(
    n, m, groups, slot, pieces,
    joined, probes, pack, unpack, gate_out, up_out, hidden,
    loaded, packed, landed, stage, acc, others,
    load_sem, send_sem, recv_sem, own_sem, out_sem, ysend_sem, yrecv_sem,
):
    layers, block_rows, cycles, _ = joined.shape
    width = loaded.shape[-1]
    half = block_rows // 2
    rows_own = n * groups * half
    me = lax.axis_index("row")
    mine = lax.axis_index("col")
    chunks = layers * pieces

    def load(c):
        return pltpu.make_async_copy(
            joined.at[c // pieces, :, :, pl.ds((c % pieces) * width, width)], loaded.at[c], load_sem.at[c]
        )

    for c in range(chunks):
        load(c).start()

    barrier = pltpu.get_barrier_semaphore()

    def greet(i, carry):
        pl.semaphore_signal(barrier, inc=1, device_id={"row": lax.rem(me + i, n)}, device_id_type=MESH)
        return carry

    lax.fori_loop(1, n, greet, 0)
    for i in range(1, m):
        pl.semaphore_signal(barrier, inc=1, device_id={"col": lax.rem(mine + i, m)}, device_id_type=MESH)
    pl.semaphore_wait(barrier, n - 1 + m - 1)

    def rows_of(q):
        return pl.ds(pl.multiple_of(q * slot, 16), slot)

    def remote(c, off):
        to = lax.rem(me + off, n)
        return pltpu.make_async_remote_copy(
            src_ref=packed.at[c, rows_of(to)],
            dst_ref=landed.at[c, rows_of(me)],
            send_sem=send_sem.at[c, off],
            recv_sem=recv_sem.at[c, off],
            device_id={"row": to},
            device_id_type=MESH,
        )

    def arrival(c, off):
        src = lax.rem(me - off + n, n)
        return pltpu.make_async_remote_copy(
            src_ref=packed.at[c, rows_of(src)],
            dst_ref=landed.at[c, rows_of(src)],
            send_sem=send_sem.at[c, off],
            recv_sem=recv_sem.at[c, off],
            device_id={"row": lax.rem(me + off, n)},
            device_id_type=MESH,
        )

    def own(c):
        return pltpu.make_async_copy(packed.at[c, rows_of(me)], landed.at[c, rows_of(me)], own_sem.at[c])

    band_out = (BAND // groups) * slot
    for c in range(chunks):
        load(c).wait()

        def pack_band(j, carry):
            band = loaded[c, :, pl.ds(pl.multiple_of(j * BAND, BAND), BAND), :]
            band = band.reshape(block_rows * BAND, width)
            moved = jnp.dot(pack[...], band, preferred_element_type=jnp.float32)
            packed[c, pl.ds(pl.multiple_of(j * band_out, 16), band_out), :] = moved.astype(jnp.bfloat16)
            return carry

        lax.fori_loop(0, cycles // BAND, pack_band, 0)

        def send(i, carry):
            remote(c, 1 + lax.rem(n // 2 - 1 + i, n - 1)).start()
            return carry

        lax.fori_loop(0, n - 1, send, 0)
        own(c).start()

    def outs(c):
        columns = pl.ds((c % pieces) * width, width)
        return [
            pltpu.make_async_copy(stage.at[c % 2, h], ref.at[c // pieces, :, columns], out_sem.at[c % 2, h])
            for h, ref in ((0, gate_out), (1, up_out))
        ]

    def partial_copy(layer, i):
        to = lax.rem(mine + i, m)
        return pltpu.make_async_remote_copy(
            src_ref=acc.at[layer, to],
            dst_ref=others.at[layer, i - 1],
            send_sem=ysend_sem.at[layer, i - 1],
            recv_sem=yrecv_sem.at[layer, i - 1],
            device_id={"col": to},
            device_id_type=MESH,
        )

    def finish(layer):
        total = acc[layer, mine]
        for i in range(1, m):
            partial_copy(layer, i).wait()
            total = total + others[layer, i - 1]
        gate = total[:, :rows_own]
        hidden[layer] = (gate / (1.0 + jnp.exp(-gate)) * total[:, rows_own:]).astype(jnp.bfloat16)

    for c in range(chunks):
        layer, piece = c // pieces, c % pieces
        if c >= 2:
            for copy in outs(c - 2):
                copy.wait()
        own(c).wait()

        def land(off, carry):
            arrival(c, off).wait_recv()
            return carry

        lax.fori_loop(1, n, land, 0)

        def unpack_peers(j, carry):
            start = pl.multiple_of(j * PEERS * slot, 16)
            moved = jnp.dot(
                unpack[...], landed[c, pl.ds(start, PEERS * slot), :], preferred_element_type=jnp.float32
            ).astype(jnp.bfloat16)
            size = PEERS * half
            for h in range(2):
                for g in range(groups):
                    first = pl.multiple_of(g * n * half + j * size, 16)
                    at = (h * groups + g) * size
                    stage[c % 2, h, pl.ds(first, size), :] = moved[at : at + size]
            return carry

        lax.fori_loop(0, n // PEERS, unpack_peers, 0)
        for copy in outs(c):
            copy.start()
        probe = probes[layer, :, piece * width : (piece + 1) * width]
        for h in range(2):
            part = lax.dot_general(
                probe, stage[c % 2, h], (((1,), (1,)), ((), ())), preferred_element_type=jnp.float32
            ).reshape(m, -1, rows_own)
            span = slice(h * rows_own, (h + 1) * rows_own)
            if piece == 0:
                acc[layer, :, :, span] = part
            else:
                acc[layer, :, :, span] += part
        if piece == pieces - 1:
            for i in range(1, m):
                partial_copy(layer, i).start()
        if c == chunks - 2:
            for early in range(layers - 1 if pieces > 1 else 0):
                finish(early)
    for late in range(layers - 1 if pieces > 1 else 0, layers):
        finish(late)
    for c in range(max(chunks - 2, 0), chunks):
        for copy in outs(c):
            copy.wait()
    for c in range(chunks):

        def sent(off, carry):
            remote(c, off).wait_send()
            return carry

        lax.fori_loop(1, n, sent, 0)


def per_device(joined, probes):
    layers, cycles, _, block_rows, columns = joined.shape
    n, m = lax.axis_size("row"), lax.axis_size("col")
    groups = cycles // n
    slot = -(-groups * block_rows // 16) * 16
    width = min(columns, 512)
    pieces = columns // width
    chunks = layers * pieces
    half = block_rows // 2
    rows_own = n * groups * half
    tokens = probes.shape[1]
    by_row = joined.transpose(0, 3, 2, 1, 4).reshape(layers, block_rows, cycles, columns)
    pack = jnp.asarray(pack_matrix(groups, block_rows, slot), jnp.bfloat16)
    unpack = jnp.asarray(unpack_matrix(groups, block_rows, slot), jnp.bfloat16)
    vmem = pl.BlockSpec(memory_space=pltpu.VMEM)
    anywhere = pl.BlockSpec(memory_space=pl.ANY)
    share = tokens // m
    weight = jax.ShapeDtypeStruct((layers, rows_own, columns), jnp.bfloat16)
    return pl.pallas_call(
        functools.partial(kernel, n, m, groups, slot, pieces),
        out_shape=(weight, weight, jax.ShapeDtypeStruct((layers, share, rows_own), jnp.bfloat16)),
        in_specs=[anywhere, vmem, vmem, vmem],
        out_specs=(anywhere, anywhere, vmem),
        scratch_shapes=[
            pltpu.VMEM((chunks, block_rows, cycles, width), jnp.bfloat16),
            pltpu.VMEM((chunks, n * slot, width), jnp.bfloat16),
            pltpu.VMEM((chunks, n * slot, width), jnp.bfloat16),
            pltpu.VMEM((2, 2, rows_own, width), jnp.bfloat16),
            pltpu.VMEM((layers, m, share, 2 * rows_own), jnp.float32),
            pltpu.VMEM((layers, max(m - 1, 1), share, 2 * rows_own), jnp.float32),
            pltpu.SemaphoreType.DMA((chunks,)),
            pltpu.SemaphoreType.DMA((chunks, n)),
            pltpu.SemaphoreType.DMA((chunks, n)),
            pltpu.SemaphoreType.DMA((chunks,)),
            pltpu.SemaphoreType.DMA((2, 2)),
            pltpu.SemaphoreType.DMA((layers, max(m - 1, 1))),
            pltpu.SemaphoreType.DMA((layers, max(m - 1, 1))),
        ],
        compiler_params=pltpu.CompilerParams(
            collective_id=0, has_side_effects=True, vmem_limit_bytes=62 * 2**20
        ),
        name="redistribute",
    )(by_row, probes, pack, unpack)


def solution(mesh):
    in_specs = (P(None, None, "row", None, "col"), P(None, None, "col"))
    out_specs = (P(None, "row", "col"), P(None, "row", "col"), P(None, "col", "row"))
    return jax.shard_map(
        per_device, mesh=mesh, in_specs=in_specs, out_specs=out_specs, check_vma=False
    )
```

```python
import functools

import jax
import jax.numpy as jnp
import numpy as np
from jax import lax
from jax.experimental import pallas as pl
from jax.experimental.pallas import tpu as pltpu
from jax.sharding import PartitionSpec as P

MESH = pl.DeviceIdType.MESH
BAND = 16
PEERS = 8


def pack_matrix(groups, block_rows, slot):
    half = block_rows // 2
    dests = BAND // groups
    out = np.zeros((dests * slot, block_rows * BAND), np.float32)
    for q in range(dests):
        for h in range(2):
            for g in range(groups):
                for r in range(half):
                    out[q * slot + (h * groups + g) * half + r, (2 * r + h) * BAND + q * groups + g] = 1
    return out


def unpack_matrix(groups, block_rows, slot):
    half = block_rows // 2
    out = np.zeros((2 * groups * PEERS * half, PEERS * slot), np.float32)
    for h in range(2):
        for g in range(groups):
            for p in range(PEERS):
                for r in range(half):
                    out[((h * groups + g) * PEERS + p) * half + r, p * slot + (h * groups + g) * half + r] = 1
    return out


def kernel(
    n, m, groups, slot, pieces,
    joined, probes, pack, unpack, gate_out, up_out, hidden, *rest,
):
    partial_outs = rest[:m]
    loaded, packed, landed, stage, acc, others = rest[m : m + 6]
    load_sem, send_sem, recv_sem, own_sem, out_sem, ysend_sem, yrecv_sem, part_sem = rest[m + 6 :]
    layers, block_rows, cycles, _ = joined.shape
    width = loaded.shape[-1]
    half = block_rows // 2
    rows_own = n * groups * half
    me = lax.axis_index("row")
    mine = lax.axis_index("col")
    chunks = layers * pieces

    def load(c):
        return pltpu.make_async_copy(
            joined.at[c // pieces, :, :, pl.ds((c % pieces) * width, width)], loaded.at[c], load_sem.at[c]
        )

    for c in range(chunks):
        load(c).start()

    barrier = pltpu.get_barrier_semaphore()

    def greet(i, carry):
        pl.semaphore_signal(barrier, inc=1, device_id={"row": lax.rem(me + i, n)}, device_id_type=MESH)
        return carry

    lax.fori_loop(1, n, greet, 0)
    for i in range(1, m):
        pl.semaphore_signal(barrier, inc=1, device_id={"col": lax.rem(mine + i, m)}, device_id_type=MESH)
    pl.semaphore_wait(barrier, n - 1 + m - 1)

    def rows_of(q):
        return pl.ds(pl.multiple_of(q * slot, 16), slot)

    def remote(c, off):
        to = lax.rem(me + off, n)
        return pltpu.make_async_remote_copy(
            src_ref=packed.at[c, rows_of(to)],
            dst_ref=landed.at[c, rows_of(me)],
            send_sem=send_sem.at[c, off],
            recv_sem=recv_sem.at[c, off],
            device_id={"row": to},
            device_id_type=MESH,
        )

    def arrival(c, off):
        src = lax.rem(me - off + n, n)
        return pltpu.make_async_remote_copy(
            src_ref=packed.at[c, rows_of(src)],
            dst_ref=landed.at[c, rows_of(src)],
            send_sem=send_sem.at[c, off],
            recv_sem=recv_sem.at[c, off],
            device_id={"row": lax.rem(me + off, n)},
            device_id_type=MESH,
        )

    def own(c):
        return pltpu.make_async_copy(packed.at[c, rows_of(me)], landed.at[c, rows_of(me)], own_sem.at[c])

    band_out = (BAND // groups) * slot
    for c in range(chunks):
        load(c).wait()

        def pack_band(j, carry):
            band = loaded[c, :, pl.ds(pl.multiple_of(j * BAND, BAND), BAND), :]
            band = band.reshape(block_rows * BAND, width)
            moved = jnp.dot(pack[...], band, preferred_element_type=jnp.float32)
            packed[c, pl.ds(pl.multiple_of(j * band_out, 16), band_out), :] = moved.astype(jnp.bfloat16)
            return carry

        lax.fori_loop(0, cycles // BAND, pack_band, 0)

        def send(i, carry):
            remote(c, 1 + lax.rem(n // 2 - 1 + i, n - 1)).start()
            return carry

        lax.fori_loop(0, n - 1, send, 0)
        own(c).start()

    def outs(c):
        columns = pl.ds((c % pieces) * width, width)
        return [
            pltpu.make_async_copy(stage.at[c % 2, h], ref.at[c // pieces, :, columns], out_sem.at[c % 2, h])
            for h, ref in ((0, gate_out), (1, up_out))
        ]

    def partial_copy(layer, i):
        to = lax.rem(mine + i, m)
        return pltpu.make_async_remote_copy(
            src_ref=acc.at[layer, to],
            dst_ref=others.at[layer, i - 1],
            send_sem=ysend_sem.at[layer, i - 1],
            recv_sem=yrecv_sem.at[layer, i - 1],
            device_id={"col": to},
            device_id_type=MESH,
        )

    def finish(layer):
        total = acc[layer, mine]
        for i in range(1, m):
            partial_copy(layer, i).wait()
            total = total + others[layer, i - 1]
        gate = total[:, :rows_own]
        hidden[layer] = (gate / (1.0 + jnp.exp(-gate)) * total[:, rows_own:]).astype(jnp.bfloat16)

    for c in range(chunks):
        layer, piece = c // pieces, c % pieces
        if c >= 2:
            for copy in outs(c - 2):
                copy.wait()
        own(c).wait()

        def land(off, carry):
            arrival(c, off).wait_recv()
            return carry

        lax.fori_loop(1, n, land, 0)

        def unpack_peers(j, carry):
            start = pl.multiple_of(j * PEERS * slot, 16)
            moved = jnp.dot(
                unpack[...], landed[c, pl.ds(start, PEERS * slot), :], preferred_element_type=jnp.float32
            ).astype(jnp.bfloat16)
            size = PEERS * half
            for h in range(2):
                for g in range(groups):
                    first = pl.multiple_of(g * n * half + j * size, 16)
                    at = (h * groups + g) * size
                    stage[c % 2, h, pl.ds(first, size), :] = moved[at : at + size]
            return carry

        lax.fori_loop(0, n // PEERS, unpack_peers, 0)
        for copy in outs(c):
            copy.start()
        probe = probes[layer, :, piece * width : (piece + 1) * width]
        for h in range(2):
            part = lax.dot_general(
                probe, stage[c % 2, h], (((1,), (1,)), ((), ())), preferred_element_type=jnp.float32
            ).reshape(m, -1, rows_own)
            span = slice(h * rows_own, (h + 1) * rows_own)
            if piece == 0:
                acc[layer, :, :, span] = part
            else:
                acc[layer, :, :, span] += part
        if piece == pieces - 1 and layer < layers - 1:
            for i in range(1, m):
                partial_copy(layer, i).start()
        if c == chunks - 2:
            for early in range(layers - 1 if pieces > 1 else 0):
                finish(early)
    hand_over = [
        pltpu.make_async_copy(acc.at[layers - 1, lax.rem(mine + i, m)], partial_outs[i], part_sem.at[i])
        for i in range(m)
    ]
    for copy in hand_over:
        copy.start()
    for late in range(layers - 1 if pieces > 1 else 0, layers - 1):
        finish(late)
    for copy in hand_over:
        copy.wait()
    for c in range(max(chunks - 2, 0), chunks):
        for copy in outs(c):
            copy.wait()
    for c in range(chunks):

        def sent(off, carry):
            remote(c, off).wait_send()
            return carry

        lax.fori_loop(1, n, sent, 0)


def settle(*refs):
    half = len(refs) // 2
    for source, target in zip(refs[:half], refs[half:]):
        target[...] = source[...]


def settled(*arrays):
    layers, rows, columns = arrays[0].shape
    height = rows // 2
    spec = pl.BlockSpec((1, height, columns), lambda i, j: (i, j, 0))
    moved = 2 * sum(a.size * a.dtype.itemsize for a in arrays)
    return pl.pallas_call(
        settle,
        grid=(layers, 2),
        in_specs=[spec] * len(arrays),
        out_specs=[spec] * len(arrays),
        out_shape=[jax.ShapeDtypeStruct(a.shape, a.dtype) for a in arrays],
        cost_estimate=pl.CostEstimate(flops=0, bytes_accessed=moved, transcendentals=0),
        compiler_params=pltpu.CompilerParams(vmem_limit_bytes=62 * 2**20),
        name="settle",
    )(*arrays)


def per_device(joined, probes):
    layers, cycles, _, block_rows, columns = joined.shape
    n, m = lax.axis_size("row"), lax.axis_size("col")
    groups = cycles // n
    slot = -(-groups * block_rows // 16) * 16
    width = min(columns, 512)
    pieces = columns // width
    chunks = layers * pieces
    half = block_rows // 2
    rows_own = n * groups * half
    tokens = probes.shape[1]
    by_row = joined.transpose(0, 3, 2, 1, 4).reshape(layers, block_rows, cycles, columns)
    pack = jnp.asarray(pack_matrix(groups, block_rows, slot), jnp.bfloat16)
    unpack = jnp.asarray(unpack_matrix(groups, block_rows, slot), jnp.bfloat16)
    vmem = pl.BlockSpec(memory_space=pltpu.VMEM)
    anywhere = pl.BlockSpec(memory_space=pl.ANY)
    share = tokens // m
    weight = jax.ShapeDtypeStruct((layers, rows_own, columns), jnp.bfloat16)
    early = layers - 1
    partial = jax.ShapeDtypeStruct((share, 2 * rows_own), jnp.float32)
    gate_rows, up_rows, hidden, kept, *given = pl.pallas_call(
        functools.partial(kernel, n, m, groups, slot, pieces),
        out_shape=(weight, weight, jax.ShapeDtypeStruct((early, share, rows_own), jnp.bfloat16), *[partial] * m),
        in_specs=[anywhere, vmem, vmem, vmem],
        out_specs=(anywhere, anywhere, vmem, *[anywhere] * m),
        scratch_shapes=[
            pltpu.VMEM((chunks, block_rows, cycles, width), jnp.bfloat16),
            pltpu.VMEM((chunks, n * slot, width), jnp.bfloat16),
            pltpu.VMEM((chunks, n * slot, width), jnp.bfloat16),
            pltpu.VMEM((2, 2, rows_own, width), jnp.bfloat16),
            pltpu.VMEM((layers, m, share, 2 * rows_own), jnp.float32),
            pltpu.VMEM((early, max(m - 1, 1), share, 2 * rows_own), jnp.float32),
            pltpu.SemaphoreType.DMA((chunks,)),
            pltpu.SemaphoreType.DMA((chunks, n)),
            pltpu.SemaphoreType.DMA((chunks, n)),
            pltpu.SemaphoreType.DMA((chunks,)),
            pltpu.SemaphoreType.DMA((2, 2)),
            pltpu.SemaphoreType.DMA((early, max(m - 1, 1))),
            pltpu.SemaphoreType.DMA((early, max(m - 1, 1))),
            pltpu.SemaphoreType.DMA((m,)),
        ],
        compiler_params=pltpu.CompilerParams(
            collective_id=0, has_side_effects=True, vmem_limit_bytes=62 * 2**20
        ),
        name="redistribute",
    )(by_row, probes, pack, unpack)
    total = kept
    for i, term in enumerate(given, 1):
        total = total + lax.ppermute(term, "col", [(q, (q + i) % m) for q in range(m)])
    gate = total[:, :rows_own]
    last = (jax.nn.silu(gate) * total[:, rows_own:]).astype(jnp.bfloat16)
    return *settled(gate_rows, up_rows), jnp.concatenate((hidden, last[None]), axis=0)


def solution(mesh):
    in_specs = (P(None, None, "row", None, "col"), P(None, None, "col"))
    out_specs = (P(None, "row", "col"), P(None, "row", "col"), P(None, "col", "row"))
    return jax.shard_map(
        per_device, mesh=mesh, in_specs=in_specs, out_specs=out_specs, check_vma=False
    )
```
